32 devices in a mesh: seq: 16 (over z, x, core), dp: 2 (over y).
Axes of the slice: x: 2, y: 2, z: 4, core: 2. Of those that a mesh axis runs over, the one named last changes fastest.
Arguments:
- spectrum: bfloat16 [16, 64, 2, 1025], P('seq', 'dp'), parts along dimension 1, may hold values from -6 to 6
- band_table: int32 [60, 2], replicated, may hold values from 0 to 1024, as said below
- band_weight: bfloat16 [60, 2, 64, 384], replicated, may hold values from -0.5 to 0.5
- qkv_weight: bfloat16 [2, 384, 1152], replicated, may hold values from -1.5 to 1.5
- out_weight: bfloat16 [2, 384, 384], replicated, may hold values from -0.3125 to 0.3125
- ff_in_weight: bfloat16 [2, 384, 768], replicated, may hold values from -0.3125 to 0.3125
- ff_out_weight: bfloat16 [2, 768, 384], replicated, may hold values from -0.21875 to 0.21875
- norm_gains: float32 [6, 384], replicated, may hold values from 0.1 to 1.9
Outputs:
- hidden_out: bfloat16 [16, 64, 60, 384], P('seq', 'dp'), parts along dimension 1
The draws below stay inside these ranges and needn't reach their ends.
There are 2 independent parts, one for each index of `dp`. The reference program is written for one: setup_inputs(seed, part) draws one part's arguments, and reference() takes and returns one part's arrays. A program takes and returns all parts, laid end to end along the dimension named above; an argument that names none is the same for every part. Nothing has to cross between parts.
Inputs may be any that keep to these rules, and one draw needn't show every extreme that they name: `band_table`: row n holds band n's first bin and its number of bins; each band lies inside the 1025 bins and has 2 to 64 bins, the last band exactly 64; bands intersect at low frequencies.
All inputs are finite; a program needn't handle non-finite values.
Results may differ from the reference program's by a relative error of at most 0.017.
Values may be sent and summed in bfloat16 or wider, within the bound.
A program may use at most 128 MiB of HBM per device.

```python
import math
import jax
import jax.numpy as jnp
from jax import lax

D = 384
HEADS = 8
BANDS = 60
BINS = 1025
SPAN = 64
CH = 2
FFH = 768
BATCH = 32
FRAMES = 16


def draw_band_table(key, part):
    first_key = jax.random.fold_in(key, 11)
    second_key = jax.random.fold_in(key, 23)
    index = jnp.arange(BANDS, dtype=jnp.int32)
    lower = 4 + (SPAN - 4) * index // (BANDS - 1)
    shrink = jax.random.randint(first_key, (BANDS,), 0, 1 << 20) % (lower // 2 + 1)
    widths = lower - shrink
    widths = jnp.where(index == BANDS - 1, SPAN, widths).astype(jnp.int32)
    base = (BINS - SPAN) * index * index // ((BANDS - 1) * (BANDS - 1))
    jitter = jax.random.randint(second_key, (BANDS,), 0, 4)
    starts = jnp.minimum(base + jitter, BINS - widths).astype(jnp.int32)
    return jnp.stack([starts, widths], axis=1).astype(jnp.int32)


def draw_qkv_weight(key, part):
    base = jax.random.normal(jax.random.fold_in(key, 5), (2, D, 3 * D), jnp.float32) * D ** (-0.5)
    return jnp.clip(base, -1.5, 1.5).astype(jnp.bfloat16)


def shard_levels(rng, extent, cuts, least, largest):
    def one(position, blocks):
        draws = jax.random.uniform(jax.random.fold_in(jax.random.fold_in(rng, 6), position), (blocks,), jnp.float32, least / len(cuts), largest / len(cuts))
        return jnp.repeat(jnp.exp(draws), extent[position] // blocks).reshape((-1,) + (1,) * (len(extent) - position - 1))

    gain = one(*cuts[0])
    for cut in cuts[1:]:
        gain = gain * one(*cut)
    return gain


def gaussian(key, dims, spread, most, pieces=(), kind=jnp.bfloat16):
    result = spread * jax.random.normal(key, dims, jnp.float32)
    if pieces:
        result = result * shard_levels(key, dims, pieces, -0.22, 0.18)
    return jnp.clip(result, -most, most).astype(kind)


def setup_inputs(seed: int = 0, part: int = 0) -> dict:
    arg_keys = jax.random.split(jax.random.key(seed), 9)
    part_keys = jax.random.split(jax.random.fold_in(arg_keys[8], part), 9)
    spectrum = gaussian(part_keys[0], (FRAMES, BATCH, CH, BINS), 1.0, 6.0, ((0, 16),))
    band_table = draw_band_table(jax.random.fold_in(arg_keys[8], 71), part)
    band_weight = gaussian(arg_keys[2], (BANDS, CH, SPAN, D), (CH * SPAN) ** -0.5, 0.5)
    qkv_weight = draw_qkv_weight(jax.random.fold_in(arg_keys[8], 71), part)
    out_weight = gaussian(arg_keys[4], (2, D, D), D ** -0.5, 0.3125)
    ff_in_weight = gaussian(arg_keys[5], (2, D, FFH), D ** -0.5, 0.3125)
    ff_out_weight = gaussian(arg_keys[6], (2, FFH, D), FFH ** -0.5, 0.21875)
    norm_gains = jnp.clip(1.0 + 0.18 * jax.random.normal(arg_keys[7], (6, D), jnp.float32), 0.1, 1.9)
    return dict(spectrum=spectrum, band_table=band_table, band_weight=band_weight, qkv_weight=qkv_weight, out_weight=out_weight, ff_in_weight=ff_in_weight, ff_out_weight=ff_out_weight, norm_gains=norm_gains)


EPSILON = 0.05

def normalize(values, gain_row):
    return values * lax.rsqrt(lax.optimization_barrier(jnp.mean(values * values, axis=-1, keepdims=True)) + EPSILON) * gain_row

def rotate(tensor, positions):
    half_size = tensor.shape[-1] // 2
    frequency = 10000.0 ** (-jnp.arange(half_size, dtype=jnp.float32) / half_size)
    angles = positions[..., None] * frequency
    cosine = jnp.cos(angles)
    sine_part = jnp.sin(angles)
    first_half = tensor[..., :half_size]
    second_half = tensor[..., half_size:]
    return jnp.concatenate([first_half * cosine - second_half * sine_part, second_half * cosine + first_half * sine_part], axis=-1)

def project(stream, weights, gain_row, positions):
    normed = normalize(stream.astype(jnp.float32), gain_row).astype(jnp.bfloat16)
    mixture = jnp.dot(normed, weights, preferred_element_type=jnp.float32)
    model_width = stream.shape[-1]
    head_shape = stream.shape[:-1] + (HEADS, model_width // HEADS)
    queries = rotate(mixture[..., :model_width].reshape(head_shape), positions).astype(jnp.bfloat16).reshape(stream.shape)
    key_rows = rotate(mixture[..., model_width:2 * model_width].reshape(head_shape), positions).astype(jnp.bfloat16).reshape(stream.shape)
    value_rows = mixture[..., 2 * model_width:].astype(jnp.bfloat16)
    return (queries, key_rows, value_rows)

def attend_rows(queries, key_rows, value_rows):
    row_count, length, model_width = queries.shape
    head_size = model_width // HEADS
    head_shape = (row_count, length, HEADS, head_size)
    scores = jnp.einsum('rshd,rthd->rhst', queries.reshape(head_shape).astype(jnp.float32), key_rows.reshape(head_shape).astype(jnp.float32)) / math.sqrt(head_size)
    weights = jax.nn.softmax(scores, axis=-1).astype(jnp.bfloat16)
    context = jnp.einsum('rhst,rthd->rshd', weights.astype(jnp.float32), value_rows.reshape(head_shape).astype(jnp.float32))
    return context.astype(jnp.bfloat16).reshape(row_count, length, model_width)

def attend_time(queries, key_rows, value_rows):
    swapped = (jnp.swapaxes(queries, 0, 1), jnp.swapaxes(key_rows, 0, 1), jnp.swapaxes(value_rows, 0, 1))

    def single(triple):
        return attend_rows(triple[0][None], triple[1][None], triple[2][None])[0]
    return jnp.swapaxes(lax.map(single, swapped), 0, 1)

def finish(stream, context, weights):
    return (stream.astype(jnp.float32) + jnp.dot(context, weights, preferred_element_type=jnp.float32)).astype(jnp.bfloat16)

def feed_forward(stream, weight_in, weight_out, gain_row):
    normed = normalize(stream.astype(jnp.float32), gain_row).astype(jnp.bfloat16)
    active = jax.nn.gelu(jnp.dot(normed, weight_in, preferred_element_type=jnp.float32), approximate=True).astype(jnp.bfloat16)
    return (stream.astype(jnp.float32) + jnp.dot(active, weight_out, preferred_element_type=jnp.float32)).astype(jnp.bfloat16)

def reference(spectrum, band_table, band_weight, qkv_weight, out_weight, ff_in_weight, ff_out_weight, norm_gains):
    offsets = jnp.arange(SPAN, dtype=jnp.int32)
    targets = (band_table[:, 0:1] + offsets[None, :]).astype(jnp.int32)
    valid = offsets[None, :] < band_table[:, 1:2]
    picked = jnp.take(spectrum, targets.reshape(-1), axis=3).reshape(FRAMES, BATCH, CH, BANDS, SPAN)
    picked = jnp.where(valid[None, None, None], picked, jnp.zeros((), picked.dtype))
    embedded = jnp.einsum('fbcnj,ncjd->fbnd', picked.astype(jnp.float32), band_weight.astype(jnp.float32))
    stream = normalize(embedded, norm_gains[0]).astype(jnp.bfloat16)
    band_positions = jnp.arange(BANDS, dtype=jnp.float32).reshape(1, BANDS, 1)

    def band_layer(block):
        triple = project(block, qkv_weight[0], norm_gains[1], band_positions)
        mixed_block = finish(block, attend_rows(triple[0], triple[1], triple[2]), out_weight[0])
        return feed_forward(mixed_block, ff_in_weight[0], ff_out_weight[0], norm_gains[2])
    stream = lax.map(band_layer, stream)
    frame_positions = jnp.arange(FRAMES, dtype=jnp.float32).reshape(FRAMES, 1, 1)

    def time_layer(block):
        triple = project(block, qkv_weight[1], norm_gains[3], frame_positions)
        mixed_block = finish(block, attend_time(triple[0], triple[1], triple[2]), out_weight[1])
        return feed_forward(mixed_block, ff_in_weight[1], ff_out_weight[1], norm_gains[4])
    by_batch = lax.map(time_layer, jnp.swapaxes(stream, 0, 1))
    stream = jnp.swapaxes(by_batch, 0, 1)
    return normalize(stream.astype(jnp.float32), norm_gains[5]).astype(jnp.bfloat16)
```

```python
import functools
import math

import jax
import jax.numpy as jnp
import numpy as np
from jax import lax
from jax.experimental import pallas as pl
from jax.experimental.pallas import tpu as pltpu
from jax.sharding import PartitionSpec as P

HEADS = 8
SPAN = 64


EPSILON = 0.05


def normalize(values, gain_row):
    return (
        values * lax.rsqrt(jnp.mean(values * values, axis=-1, keepdims=True) + EPSILON) * gain_row
    )


def rotate(tensor, positions):
    half_size = tensor.shape[-1] // 2
    frequency = 10000.0 ** (-jnp.arange(half_size, dtype=jnp.float32) / half_size)
    angles = positions[..., None] * frequency
    cosine = jnp.cos(angles)
    sine_part = jnp.sin(angles)
    first_half = tensor[..., :half_size]
    second_half = tensor[..., half_size:]
    return jnp.concatenate(
        [
            first_half * cosine - second_half * sine_part,
            second_half * cosine + first_half * sine_part,
        ],
        axis=-1,
    )


def project(stream, weights, gain_row, positions):
    normed = normalize(stream.astype(jnp.float32), gain_row).astype(jnp.bfloat16)
    mixture = jnp.dot(normed, weights, preferred_element_type=jnp.float32)
    model_width = stream.shape[-1]
    head_shape = stream.shape[:-1] + (HEADS, model_width // HEADS)
    queries = (
        rotate(mixture[..., :model_width].reshape(head_shape), positions)
        .astype(jnp.bfloat16)
        .reshape(stream.shape)
    )
    key_rows = (
        rotate(mixture[..., model_width : 2 * model_width].reshape(head_shape), positions)
        .astype(jnp.bfloat16)
        .reshape(stream.shape)
    )
    value_rows = mixture[..., 2 * model_width :].astype(jnp.bfloat16)
    return (queries, key_rows, value_rows)


def attend_rows(queries, key_rows, value_rows):
    row_count, length, model_width = queries.shape
    head_size = model_width // HEADS
    head_shape = (row_count, length, HEADS, head_size)
    scores = jnp.einsum(
        "rshd,rthd->rhst",
        queries.reshape(head_shape),
        key_rows.reshape(head_shape),
        preferred_element_type=jnp.float32,
    ) / math.sqrt(head_size)
    weights = jax.nn.softmax(scores, axis=-1).astype(jnp.bfloat16)
    context = jnp.einsum(
        "rhst,rthd->rshd",
        weights,
        value_rows.reshape(head_shape),
        preferred_element_type=jnp.float32,
    )
    return context.astype(jnp.bfloat16).reshape(row_count, length, model_width)


def attend_time(queries, key_rows, value_rows):
    context = attend_rows(
        jnp.swapaxes(queries, 0, 1), jnp.swapaxes(key_rows, 0, 1), jnp.swapaxes(value_rows, 0, 1)
    )
    return jnp.swapaxes(context, 0, 1)


def finish(stream, context, weights):
    return (
        stream.astype(jnp.float32) + jnp.dot(context, weights, preferred_element_type=jnp.float32)
    ).astype(jnp.bfloat16)


def feed_forward(stream, weight_in, weight_out, gain_row):
    normed = normalize(stream.astype(jnp.float32), gain_row).astype(jnp.bfloat16)
    active = jax.nn.gelu(
        jnp.dot(normed, weight_in, preferred_element_type=jnp.float32), approximate=True
    ).astype(jnp.bfloat16)
    return (
        stream.astype(jnp.float32) + jnp.dot(active, weight_out, preferred_element_type=jnp.float32)
    ).astype(jnp.bfloat16)


def flatten_items(block):
    return block.reshape(block.shape[0], block.shape[2], block.shape[3])


LANES = 128
PAIRS = HEADS // 2
WIDE = PAIRS * LANES
F32 = jnp.float32
BF16 = jnp.bfloat16
TIME_BANDS = 32
MESH = pl.DeviceIdType.MESH


def fits_batch_plan(spectrum, band_table, band_weight):
    groups = lax.axis_size("seq")
    return (
        spectrum.shape[0] == 1
        and spectrum.shape[1] % groups == 0
        and groups % 16 == 0
        and groups <= 16
        and band_table.shape[0] <= 2 * TIME_BANDS
        and band_table.shape[0] > TIME_BANDS
        and band_weight.shape[3] == HEADS * 48
    )


def rotation_tables(length, head_size, scale):
    half = head_size // 2
    frequency = 10000.0 ** (-np.arange(half, dtype=np.float64) / half)
    angles = np.arange(length, dtype=np.float64)[:, None] * frequency
    cosine = np.zeros((length, LANES), np.float32)
    sine = np.zeros((length, LANES), np.float32)
    for head in range(2):
        for part in range(2):
            at = part * 64 + head * 32
            cosine[:, at : at + half] = np.cos(angles) * scale
            sine[:, at : at + half] = np.sin(angles) * (scale if part else -scale)
    return cosine, sine


def dot(left, right):
    return jnp.dot(left, right, preferred_element_type=F32)


def rms(values, gain):
    mean = jnp.mean(values * values, axis=-1, keepdims=True)
    return values * lax.rsqrt(mean + EPSILON) * gain


def layer(x, tables, gain_a, gain_f, wqkv, wout, wfi, wfo, size, mask, low):
    rows = x.shape[0]
    blocks = rows // size
    cq, sq, ck, sk = tables
    lane = lax.broadcasted_iota(jnp.int32, (1, LANES), 1)
    first = ((lane & 32) == 0).astype(BF16)
    second = ((lane & 32) != 0).astype(BF16)
    normed = rms(x, gain_a).astype(BF16)
    mixture = dot(normed, wqkv)

    def turned(part, cosine, sine):
        swapped = pltpu.roll(part, 64, 1)
        part = part.reshape(blocks, size, LANES) * cosine[None]
        return (part + swapped.reshape(blocks, size, LANES) * sine[None]).astype(BF16)

    columns = []
    for pair in range(PAIRS):
        at = pair * LANES
        q = turned(mixture[:, at : at + LANES], cq, sq)
        k = turned(mixture[:, WIDE + at : WIDE + at + LANES], ck, sk)
        v = mixture[:, 2 * WIDE + at : 2 * WIDE + at + LANES].astype(BF16)
        pieces = []
        for block in range(blocks):
            qb = q[block]
            stacked = jnp.concatenate([qb * first, qb * second], axis=0)
            scores = lax.dot_general(
                k[block], stacked, (((1,), (1,)), ((), ())), preferred_element_type=F32
            )
            scores = jnp.where(mask, scores, low)
            scores = jnp.exp2(scores - jnp.max(scores, axis=0, keepdims=True))
            total = jnp.sum(scores, axis=0, keepdims=True)
            probs = (scores * (1.0 / total)).astype(BF16)
            mixed = lax.dot_general(
                probs,
                v[block * size : (block + 1) * size],
                (((0,), (0,)), ((), ())),
                preferred_element_type=F32,
            )
            pieces.append(jnp.where(lane < 64, mixed[:size], mixed[size:]))
        columns.append(jnp.concatenate(pieces, axis=0).astype(BF16))
    x = x + dot(jnp.concatenate(columns, axis=1), wout)
    normed = rms(x, gain_f).astype(BF16)
    u = dot(normed, wfi)
    c = math.sqrt(2.0 / math.pi)
    act = 0.5 * u * (1.0 + jnp.tanh(u * (c + (c * 0.044715) * (u * u))))
    return x + dot(act.astype(BF16), wfo)


def whole_kernel(
    groups,
    own,
    bands,
    bins,
    table,
    spectrum,
    band_weight,
    qkv,
    out_w,
    ff_in,
    ff_out,
    gains,
    cq0,
    sq0,
    ck0,
    sk0,
    cq1,
    sq1,
    ck1,
    sk1,
    out,
    arrived,
    spec,
    bw,
    raw_qkv,
    raw_out,
    wqkv,
    wout,
    wfi,
    wfo,
    x0,
    x1,
    sending,
    load_sem,
    spec_send,
    spec_recv,
    spec_own,
    send_sem,
    recv_sem,
    own_sem,
):
    me = lax.axis_index("seq")
    padded = 2 * TIME_BANDS
    frames = groups
    width = gains.shape[1]
    loads = [
        pltpu.make_async_copy(qkv, raw_qkv, load_sem.at[0]),
        pltpu.make_async_copy(out_w, raw_out, load_sem.at[1]),
        pltpu.make_async_copy(band_weight, bw, load_sem.at[2]),
        pltpu.make_async_copy(ff_in, wfi, load_sem.at[3]),
        pltpu.make_async_copy(ff_out, wfo, load_sem.at[4]),
    ]
    for load in loads:
        load.start()

    barrier = pltpu.get_barrier_semaphore()

    def greet(k, carry):
        peer = lax.rem(me + k, groups)
        pl.semaphore_signal(barrier, inc=1, device_id={"seq": peer}, device_id_type=MESH)
        return carry

    lax.fori_loop(1, groups, greet, 0)
    pl.semaphore_wait(barrier, groups - 1)

    def spec_copy(peer, slot, sem_slot):
        return pltpu.make_async_remote_copy(
            src_ref=spectrum.at[pl.ds(peer * own, own)],
            dst_ref=arrived.at[slot],
            send_sem=spec_send.at[peer],
            recv_sem=spec_recv.at[sem_slot],
            device_id={"seq": peer},
            device_id_type=MESH,
        )

    def spec_start(k, carry):
        peer = lax.rem(me + k, groups)
        spec_copy(peer, me, me).start()
        return carry

    lax.fori_loop(1, groups, spec_start, 0)
    mine = pltpu.make_async_copy(
        spectrum.at[pl.ds(me * own, own)], arrived.at[me], spec_own.at[0]
    )
    mine.start()

    col = lax.broadcasted_iota(jnp.int32, (1, WIDE), 1)
    pair, rest = col >> 7, col & 127
    part, head, at = rest >> 6, (rest >> 5) & 1, rest & 31
    source = jnp.where(at < 24, pair * 96 + head * 48 + part * 24 + at, -1)
    row = lax.broadcasted_iota(jnp.int32, (width, WIDE), 0)
    spread_qk = (row == source).astype(F32).astype(BF16)
    source = jnp.where((col & 63) < 48, (col >> 6) * 48 + (col & 63), -1)
    spread_v = (row == source).astype(F32).astype(BF16)
    col = lax.broadcasted_iota(jnp.int32, (WIDE, 1), 0)
    source = jnp.where((col & 63) < 48, (col >> 6) * 48 + (col & 63), -1)
    row = lax.broadcasted_iota(jnp.int32, (WIDE, width), 1)
    spread_o = (row == source).astype(F32).astype(BF16)
    loads[0].wait()
    loads[1].wait()
    for sub in range(2):
        for block in range(3):
            spread = spread_v if block == 2 else spread_qk
            wqkv[sub, :, block * WIDE : (block + 1) * WIDE] = dot(
                raw_qkv[sub, :, block * width : (block + 1) * width], spread
            ).astype(BF16)
        wout[sub] = dot(spread_o, raw_out[sub]).astype(BF16)

    mine.wait()

    def spec_wait(k, carry):
        peer = lax.rem(me + k, groups)
        copy = spec_copy(peer, peer, peer)
        copy.wait_send()
        copy.wait_recv()
        return carry

    lax.fori_loop(1, groups, spec_wait, 0)
    for f in range(frames):
        for b in range(own):
            both = arrived[f, b].astype(F32)
            at = b * frames + f
            spec[at : at + 1, 0:bins] = both[0:1]
            at = (own + b) * frames + f
            spec[at : at + 1, 0:bins] = both[1:2]

    loads[2].wait()
    lane = lax.broadcasted_iota(jnp.int32, (1, LANES), 1)
    gain0 = gains[0:1, :]

    def scatter(n, values):
        for b in range(own):
            for piece in range(width // LANES):
                x0[piece, pl.ds(b * frames * padded + n, frames, stride=padded), :] = values[
                    b * frames : (b + 1) * frames, piece * LANES : (piece + 1) * LANES
                ]

    def embed(n, carry):
        start = table[n, 0]
        count = table[n, 1]
        amount = jnp.full((1, LANES), start, jnp.int32)
        tiles = [
            spec[:, i * LANES : (i + 1) * LANES] for i in range(spec.shape[1] // LANES)
        ]
        for bit in range(3, -1, -1):
            step = 1 << bit
            if len(tiles) > step:
                chosen = (amount & (LANES << bit)) != 0
                tiles = [
                    jnp.where(chosen, tiles[i + step], tiles[i]) if i + step < len(tiles) else tiles[i]
                    for i in range(min(len(tiles), step + 1))
                ]
        window = jnp.concatenate(tiles[:2], axis=1)
        for bit in range(7):
            moved = pltpu.roll(window, 256 - (1 << bit), 1)
            chosen = (jnp.full((1, 256), start, jnp.int32) & (1 << bit)) != 0
            window = jnp.where(chosen, moved, window)
        count_rows = own * frames
        high = pltpu.roll(window[count_rows:, :LANES], 64, 1)
        picked = jnp.where(lane < 64, window[:count_rows, :LANES], high)
        picked = jnp.where((lane & 63) < count, picked, 0.0).astype(BF16)
        scatter(n, rms(dot(picked, bw[n]), gain0))
        return carry

    lax.fori_loop(0, bands, embed, 0, unroll=4)
    for n in range(bands, padded):
        scatter(n, jnp.zeros((own * frames, width), F32))

    loads[3].wait()
    loads[4].wait()
    rows = 512
    band_mask = lax.broadcasted_iota(jnp.int32, (padded, 2 * padded), 0) < bands
    small = 8 * frames
    time_mask = (lax.broadcasted_iota(jnp.int32, (small, 2 * small), 0) & 7) == (
        lax.broadcasted_iota(jnp.int32, (small, 2 * small), 1) & 7
    )

    def out_copy(peer, b, part, slot):
        return pltpu.make_async_remote_copy(
            src_ref=sending.at[b, part, peer],
            dst_ref=out.at[slot * own + b, pl.ds(part * TIME_BANDS, TIME_BANDS)],
            send_sem=send_sem.at[b, part, peer],
            recv_sem=recv_sem.at[b, part, slot],
            device_id={"seq": peer},
            device_id_type=MESH,
        )

    def own_copy(b, part):
        return pltpu.make_async_copy(
            sending.at[b, part, me],
            out.at[me * own + b, pl.ds(part * TIME_BANDS, TIME_BANDS)],
            own_sem.at[b, part],
        )

    def one_row(b, carry):
        def band_chunk(chunk, carry):
            at = pl.multiple_of(b * frames * padded + chunk * rows, rows)
            x = jnp.concatenate(
                [x0[piece, pl.ds(at, rows), :] for piece in range(width // LANES)], axis=1
            )
            x = layer(
                x,
                (cq0[...], sq0[...], ck0[...], sk0[...]),
                gains[1:2, :],
                gains[2:3, :],
                wqkv[0],
                wout[0],
                wfi[0],
                wfo[0],
                padded,
                band_mask,
                -1e30,
            )
            count = rows // padded
            x1[b, pl.ds(chunk * count, count)] = x.reshape(count, padded, width)
            return carry

        lax.fori_loop(0, frames * padded // rows, band_chunk, 0)

        def time_chunk(part, carry):
            n0 = part * TIME_BANDS
            x = jnp.concatenate(
                [
                    x1[b, :, pl.ds(pl.multiple_of(n0 + 8 * g, 8), 8), :].reshape(small, width)
                    for g in range(TIME_BANDS // 8)
                ],
                axis=0,
            )
            x = layer(
                x,
                (cq1[...], sq1[...], ck1[...], sk1[...]),
                gains[3:4, :],
                gains[4:5, :],
                wqkv[1],
                wout[1],
                wfi[1],
                wfo[1],
                small,
                time_mask,
                -1e30,
            )
            y = rms(x, gains[5:6, :])
            y = jnp.concatenate(
                [
                    y[g * small : (g + 1) * small].reshape(frames, 8, width)
                    for g in range(TIME_BANDS // 8)
                ],
                axis=1,
            )
            sending[b, part] = y.astype(BF16)

            def start(k, carry):
                peer = lax.rem(me + k, groups)
                out_copy(peer, b, part, me).start()
                return carry

            lax.fori_loop(1, groups, start, 0)
            own_copy(b, part).start()
            return carry

        lax.fori_loop(0, padded // TIME_BANDS, time_chunk, 0)
        return carry

    lax.fori_loop(0, own, one_row, 0)

    def finish_all(i, carry):
        b, part = i // 2, lax.rem(i, 2)

        def one(k, carry):
            peer = lax.rem(me + k, groups)
            copy = out_copy(peer, b, part, peer)
            copy.wait_send()
            copy.wait_recv()
            return carry

        lax.fori_loop(1, groups, one, 0)
        own_copy(b, part).wait()
        return carry

    lax.fori_loop(0, own * 2, finish_all, 0)


def batch_plan(
    spectrum,
    band_table,
    band_weight,
    qkv_weight,
    out_weight,
    ff_in_weight,
    ff_out_weight,
    norm_gains,
):
    groups = lax.axis_size("seq")
    _, batch_size, channels, bins = spectrum.shape
    bands = band_table.shape[0]
    width = band_weight.shape[3]
    hidden = ff_in_weight.shape[2]
    own = batch_size // groups
    padded = 2 * TIME_BANDS
    bins_padded = -(-bins // LANES) * LANES
    head_size = width // HEADS
    scale = math.log2(math.e) / math.sqrt(head_size)
    tables = []
    for length, repeat in ((padded, 1), (groups, 8)):
        for factor in (scale, 1.0):
            for piece in rotation_tables(length, head_size, factor):
                tables.append(np.repeat(piece, repeat, axis=0))
    vmem = pl.BlockSpec(memory_space=pltpu.VMEM)
    anywhere = pl.BlockSpec(memory_space=pl.ANY)
    dma = pltpu.SemaphoreType.DMA
    out = pl.pallas_call(
        functools.partial(whole_kernel, groups, own, bands, bins),
        out_shape=jax.ShapeDtypeStruct((batch_size, padded, width), BF16),
        in_specs=[pl.BlockSpec(memory_space=pltpu.SMEM)] + [anywhere] * 6 + [vmem] * 9,
        out_specs=anywhere,
        scratch_shapes=[
            pltpu.VMEM((groups, own, channels, bins), BF16),
            pltpu.VMEM((channels * own * groups, bins_padded), F32),
            pltpu.VMEM((bands, channels * SPAN, width), BF16),
            pltpu.VMEM((2, width, 3 * width), BF16),
            pltpu.VMEM((2, width, width), BF16),
            pltpu.VMEM((2, width, 3 * WIDE), BF16),
            pltpu.VMEM((2, WIDE, width), BF16),
            pltpu.VMEM((2, width, hidden), BF16),
            pltpu.VMEM((2, hidden, width), BF16),
            pltpu.VMEM((width // LANES, own * groups * padded, LANES), F32),
            pltpu.VMEM((own, groups, padded, width), F32),
            pltpu.VMEM((own, 2, groups, TIME_BANDS, width), BF16),
            dma((5,)),
            dma((groups,)),
            dma((groups,)),
            dma((1,)),
            dma((own, 2, groups)),
            dma((own, 2, groups)),
            dma((own, 2)),
        ],
        compiler_params=pltpu.CompilerParams(collective_id=0, has_side_effects=True),
    )(
        band_table,
        spectrum.reshape(batch_size, channels, bins),
        band_weight.reshape(bands, channels * SPAN, width),
        qkv_weight,
        out_weight,
        ff_in_weight,
        ff_out_weight,
        norm_gains,
        *[jnp.asarray(t) for t in tables],
    )
    return out[None, :, :bands]


def body(
    spectrum,
    band_table,
    band_weight,
    qkv_weight,
    out_weight,
    ff_in_weight,
    ff_out_weight,
    norm_gains,
):
    frame_count, batch_size, channel_count, bin_count = spectrum.shape
    band_count = band_table.shape[0]
    if fits_batch_plan(spectrum, band_table, band_weight):
        return batch_plan(
            spectrum,
            band_table,
            band_weight,
            qkv_weight,
            out_weight,
            ff_in_weight,
            ff_out_weight,
            norm_gains,
        )
    offsets = jnp.arange(SPAN, dtype=jnp.int32)
    targets = (band_table[:, 0:1] + offsets[None, :]).reshape(-1)
    valid = (offsets[None, :] < band_table[:, 1:2]).reshape(-1)
    chosen = (
        (jnp.arange(bin_count, dtype=jnp.int32)[:, None] == targets[None, :]) & valid[None, :]
    ).astype(jnp.bfloat16)
    features = jnp.einsum(
        "fbcq,qm->fbcm", spectrum, chosen, preferred_element_type=jnp.float32
    ).astype(jnp.bfloat16)
    features = features.reshape(frame_count, batch_size, channel_count, band_count, SPAN)
    embedded = jnp.einsum(
        "fbcnj,ncjd->fbnd", features, band_weight, preferred_element_type=jnp.float32
    )
    model_width = embedded.shape[-1]
    stream = normalize(embedded, norm_gains[0]).astype(jnp.bfloat16)
    stream = stream.reshape(frame_count * batch_size, band_count, model_width)
    band_positions = jnp.arange(band_count, dtype=jnp.float32).reshape(1, band_count, 1)
    triple = project(stream, qkv_weight[0], norm_gains[1], band_positions)
    stream = finish(stream, attend_rows(triple[0], triple[1], triple[2]), out_weight[0])
    stream = feed_forward(stream, ff_in_weight[0], ff_out_weight[0], norm_gains[2])
    groups = lax.axis_size("seq")
    pair_count = batch_size * band_count
    per_group = pair_count // groups
    stream = stream.reshape(frame_count, groups, per_group, model_width)
    block = lax.all_to_all(stream, "seq", split_axis=1, concat_axis=0, tiled=True)
    flat = flatten_items(block)
    length = flat.shape[0]
    frame_positions = jnp.arange(length, dtype=jnp.float32).reshape(length, 1, 1)
    parts = project(flat, qkv_weight[1], norm_gains[3], frame_positions)
    mixed_block = finish(flat, attend_time(parts[0], parts[1], parts[2]), out_weight[1])
    result_block = feed_forward(mixed_block, ff_in_weight[1], ff_out_weight[1], norm_gains[4])
    regrouped = result_block.reshape(block.shape)
    stream = lax.all_to_all(regrouped, "seq", split_axis=0, concat_axis=1, tiled=True)
    stream = stream.reshape(frame_count, pair_count, model_width)
    result = normalize(stream.astype(jnp.float32), norm_gains[5]).astype(jnp.bfloat16)
    return result.reshape(frame_count, batch_size, band_count, model_width)


def solution(mesh):
    in_specs = (P("seq", "dp", None, None), P(), P(), P(), P(), P(), P(), P())
    out_specs = P("seq", "dp", None, None)
    return jax.shard_map(body, mesh=mesh, in_specs=in_specs, out_specs=out_specs, check_vma=False)
```

```python
import functools
import math

import jax
import jax.numpy as jnp
import numpy as np
from jax import lax
from jax.experimental import pallas as pl
from jax.experimental.pallas import tpu as pltpu
from jax.sharding import PartitionSpec as P

HEADS = 8
SPAN = 64


EPSILON = 0.05


def normalize(values, gain_row):
    return (
        values * lax.rsqrt(jnp.mean(values * values, axis=-1, keepdims=True) + EPSILON) * gain_row
    )


def rotate(tensor, positions):
    half_size = tensor.shape[-1] // 2
    frequency = 10000.0 ** (-jnp.arange(half_size, dtype=jnp.float32) / half_size)
    angles = positions[..., None] * frequency
    cosine = jnp.cos(angles)
    sine_part = jnp.sin(angles)
    first_half = tensor[..., :half_size]
    second_half = tensor[..., half_size:]
    return jnp.concatenate(
        [
            first_half * cosine - second_half * sine_part,
            second_half * cosine + first_half * sine_part,
        ],
        axis=-1,
    )


def project(stream, weights, gain_row, positions):
    normed = normalize(stream.astype(jnp.float32), gain_row).astype(jnp.bfloat16)
    mixture = jnp.dot(normed, weights, preferred_element_type=jnp.float32)
    model_width = stream.shape[-1]
    head_shape = stream.shape[:-1] + (HEADS, model_width // HEADS)
    queries = (
        rotate(mixture[..., :model_width].reshape(head_shape), positions)
        .astype(jnp.bfloat16)
        .reshape(stream.shape)
    )
    key_rows = (
        rotate(mixture[..., model_width : 2 * model_width].reshape(head_shape), positions)
        .astype(jnp.bfloat16)
        .reshape(stream.shape)
    )
    value_rows = mixture[..., 2 * model_width :].astype(jnp.bfloat16)
    return (queries, key_rows, value_rows)


def attend_rows(queries, key_rows, value_rows):
    row_count, length, model_width = queries.shape
    head_size = model_width // HEADS
    head_shape = (row_count, length, HEADS, head_size)
    scores = jnp.einsum(
        "rshd,rthd->rhst",
        queries.reshape(head_shape),
        key_rows.reshape(head_shape),
        preferred_element_type=jnp.float32,
    ) / math.sqrt(head_size)
    weights = jax.nn.softmax(scores, axis=-1).astype(jnp.bfloat16)
    context = jnp.einsum(
        "rhst,rthd->rshd",
        weights,
        value_rows.reshape(head_shape),
        preferred_element_type=jnp.float32,
    )
    return context.astype(jnp.bfloat16).reshape(row_count, length, model_width)


def attend_time(queries, key_rows, value_rows):
    context = attend_rows(
        jnp.swapaxes(queries, 0, 1), jnp.swapaxes(key_rows, 0, 1), jnp.swapaxes(value_rows, 0, 1)
    )
    return jnp.swapaxes(context, 0, 1)


def finish(stream, context, weights):
    return (
        stream.astype(jnp.float32) + jnp.dot(context, weights, preferred_element_type=jnp.float32)
    ).astype(jnp.bfloat16)


def feed_forward(stream, weight_in, weight_out, gain_row):
    normed = normalize(stream.astype(jnp.float32), gain_row).astype(jnp.bfloat16)
    active = jax.nn.gelu(
        jnp.dot(normed, weight_in, preferred_element_type=jnp.float32), approximate=True
    ).astype(jnp.bfloat16)
    return (
        stream.astype(jnp.float32) + jnp.dot(active, weight_out, preferred_element_type=jnp.float32)
    ).astype(jnp.bfloat16)


def flatten_items(block):
    return block.reshape(block.shape[0], block.shape[2], block.shape[3])


LANES = 128
PAIRS = HEADS // 2
WIDE = PAIRS * LANES
F32 = jnp.float32
BF16 = jnp.bfloat16
TIME_BANDS = 32
MESH = pl.DeviceIdType.MESH


def fits_batch_plan(spectrum, band_table, band_weight):
    groups = lax.axis_size("seq")
    return (
        spectrum.shape[0] == 1
        and spectrum.shape[1] % groups == 0
        and groups % 16 == 0
        and groups <= 16
        and band_table.shape[0] <= 2 * TIME_BANDS
        and band_table.shape[0] > TIME_BANDS
        and band_table.shape[0] % 4 == 0
        and SPAN == 64
        and spectrum.shape[2] == 2
        and band_weight.shape[3] == HEADS * 48
    )


def rotation_tables(length, head_size, scale):
    half = head_size // 2
    frequency = 10000.0 ** (-np.arange(half, dtype=np.float64) / half)
    angles = np.arange(length, dtype=np.float64)[:, None] * frequency
    cosine = np.zeros((length, LANES), np.float32)
    sine = np.zeros((length, LANES), np.float32)
    for head in range(2):
        for part in range(2):
            at = part * 64 + head * 32
            cosine[:, at : at + half] = np.cos(angles) * scale
            sine[:, at : at + half] = np.sin(angles) * (scale if part else -scale)
    return cosine, sine


def dot(left, right):
    return jnp.dot(left, right, preferred_element_type=F32)


def rms(values, gain):
    mean = jnp.mean(values * values, axis=-1, keepdims=True)
    return values * lax.rsqrt(mean + EPSILON) * gain


def layer(x, tables, gain_a, gain_f, wqkv, wout, wfi, wfo, size, mask, low):
    rows = x.shape[0]
    blocks = rows // size
    cq, sq, ck, sk = tables
    lane = lax.broadcasted_iota(jnp.int32, (1, LANES), 1)
    first = ((lane & 32) == 0).astype(BF16)
    second = ((lane & 32) != 0).astype(BF16)
    normed = rms(x, gain_a).astype(BF16)
    mixture = dot(normed, wqkv)

    def turned(part, cosine, sine):
        swapped = pltpu.roll(part, 64, 1)
        part = part.reshape(blocks, size, LANES) * cosine[None]
        return (part + swapped.reshape(blocks, size, LANES) * sine[None]).astype(BF16)

    columns = []
    for pair in range(PAIRS):
        at = pair * LANES
        q = turned(mixture[:, at : at + LANES], cq, sq)
        k = turned(mixture[:, WIDE + at : WIDE + at + LANES], ck, sk)
        v = mixture[:, 2 * WIDE + at : 2 * WIDE + at + LANES].astype(BF16)
        pieces = []
        for block in range(blocks):
            qb = q[block]
            stacked = jnp.concatenate([qb * first, qb * second], axis=0)
            scores = lax.dot_general(
                k[block], stacked, (((1,), (1,)), ((), ())), preferred_element_type=F32
            )
            scores = jnp.where(mask, scores, low)
            scores = jnp.exp2(scores - jnp.max(scores, axis=0, keepdims=True))
            total = jnp.sum(scores, axis=0, keepdims=True)
            probs = (scores * (1.0 / total)).astype(BF16)
            mixed = lax.dot_general(
                probs,
                v[block * size : (block + 1) * size],
                (((0,), (0,)), ((), ())),
                preferred_element_type=F32,
            )
            pieces.append(jnp.where(lane < 64, mixed[:size], mixed[size:]))
        columns.append(jnp.concatenate(pieces, axis=0).astype(BF16))
    x = x + dot(jnp.concatenate(columns, axis=1), wout)
    normed = rms(x, gain_f).astype(BF16)
    u = dot(normed, wfi)
    c = math.sqrt(2.0 / math.pi)
    act = 0.5 * u * (1.0 + jnp.tanh(u * (c + (c * 0.044715) * (u * u))))
    return x + dot(act.astype(BF16), wfo)


def whole_kernel(
    groups,
    own,
    bands,
    bins,
    table,
    spectrum,
    band_weight,
    qkv,
    out_w,
    ff_in,
    ff_out,
    gains,
    cq0,
    sq0,
    ck0,
    sk0,
    cq1,
    sq1,
    ck1,
    sk1,
    out,
    arrived,
    spec,
    feats,
    bw,
    raw_qkv,
    raw_out,
    wqkv,
    wout,
    wfi,
    wfo,
    x0,
    x1,
    sending,
    load_sem,
    spec_send,
    spec_recv,
    spec_own,
    send_sem,
    recv_sem,
    own_sem,
):
    me = lax.axis_index("seq")
    padded = 2 * TIME_BANDS
    frames = groups
    width = gains.shape[1]
    loads = [
        pltpu.make_async_copy(qkv, raw_qkv, load_sem.at[0]),
        pltpu.make_async_copy(out_w, raw_out, load_sem.at[1]),
        pltpu.make_async_copy(band_weight, bw, load_sem.at[2]),
        pltpu.make_async_copy(ff_in, wfi, load_sem.at[3]),
        pltpu.make_async_copy(ff_out, wfo, load_sem.at[4]),
    ]
    for load in loads:
        load.start()

    barrier = pltpu.get_barrier_semaphore()

    def greet(k, carry):
        peer = lax.rem(me + k, groups)
        pl.semaphore_signal(barrier, inc=1, device_id={"seq": peer}, device_id_type=MESH)
        return carry

    lax.fori_loop(1, groups, greet, 0)
    pl.semaphore_wait(barrier, groups - 1)

    def spec_copy(peer, slot, sem_slot):
        return pltpu.make_async_remote_copy(
            src_ref=spectrum.at[pl.ds(peer * own, own)],
            dst_ref=arrived.at[slot],
            send_sem=spec_send.at[peer],
            recv_sem=spec_recv.at[sem_slot],
            device_id={"seq": peer},
            device_id_type=MESH,
        )

    def spec_start(k, carry):
        peer = lax.rem(me + k, groups)
        spec_copy(peer, me, me).start()
        return carry

    lax.fori_loop(1, groups, spec_start, 0)
    tail = bins // LANES * LANES
    spec[:, tail:] = jnp.zeros((spec.shape[0], spec.shape[1] - tail), F32)
    mine = pltpu.make_async_copy(
        spectrum.at[pl.ds(me * own, own)], arrived.at[me], spec_own.at[0]
    )
    mine.start()

    col = lax.broadcasted_iota(jnp.int32, (1, WIDE), 1)
    pair, rest = col >> 7, col & 127
    part, head, at = rest >> 6, (rest >> 5) & 1, rest & 31
    source = jnp.where(at < 24, pair * 96 + head * 48 + part * 24 + at, -1)
    row = lax.broadcasted_iota(jnp.int32, (width, WIDE), 0)
    spread_qk = (row == source).astype(F32).astype(BF16)
    source = jnp.where((col & 63) < 48, (col >> 6) * 48 + (col & 63), -1)
    spread_v = (row == source).astype(F32).astype(BF16)
    col = lax.broadcasted_iota(jnp.int32, (WIDE, 1), 0)
    source = jnp.where((col & 63) < 48, (col >> 6) * 48 + (col & 63), -1)
    row = lax.broadcasted_iota(jnp.int32, (WIDE, width), 1)
    spread_o = (row == source).astype(F32).astype(BF16)
    loads[0].wait()
    loads[1].wait()
    for sub in range(2):
        for block in range(3):
            spread = spread_v if block == 2 else spread_qk
            wqkv[sub, :, block * WIDE : (block + 1) * WIDE] = dot(
                raw_qkv[sub, :, block * width : (block + 1) * width], spread
            ).astype(BF16)
        wout[sub] = dot(spread_o, raw_out[sub]).astype(BF16)

    mine.wait()

    def spec_wait(k, carry):
        peer = lax.rem(me + k, groups)
        copy = spec_copy(peer, peer, peer)
        copy.wait_send()
        copy.wait_recv()
        return carry

    lax.fori_loop(1, groups, spec_wait, 0)
    for f in range(frames):
        for b in range(own):
            both = arrived[f, b].astype(F32)
            at = b * frames + f
            spec[at : at + 1, 0:bins] = both[0:1]
            at = (own + b) * frames + f
            spec[at : at + 1, 0:bins] = both[1:2]

    loads[2].wait()
    lane = lax.broadcasted_iota(jnp.int32, (1, LANES), 1)
    gain0 = gains[0:1, :]

    def scatter(n, values):
        for b in range(own):
            for piece in range(width // LANES):
                x0[piece, pl.ds(b * frames * padded + n, frames, stride=padded), :] = values[
                    b * frames : (b + 1) * frames, piece * LANES : (piece + 1) * LANES
                ]

    quad = 4 * SPAN
    offset = lax.broadcasted_iota(jnp.int32, (1, quad), 1) & (SPAN - 1)
    owner = lax.broadcasted_iota(jnp.int32, (1, quad), 1) // SPAN
    lines = spec[...].astype(BF16)
    bin_row = lax.broadcasted_iota(jnp.int32, (spec.shape[1], quad), 0)

    def pick(m, carry):
        target = jnp.full((1, quad), -1, jnp.int32)
        for i in range(4):
            start = jnp.full((1, quad), table[0, 4 * m + i], jnp.int32)
            count = jnp.full((1, quad), table[1, 4 * m + i], jnp.int32)
            inside = (owner == i) & (offset < count)
            target = jnp.where(inside, start + offset, target)
        chosen = (bin_row == target).astype(F32).astype(BF16)
        feats[m] = dot(lines, chosen)
        return carry

    lax.fori_loop(0, bands // 4, pick, 0, unroll=3)
    half = own * frames

    def embed(m, carry):
        for i in range(2):
            low = feats[m, :half, i * LANES : (i + 1) * LANES]
            high = feats[m, half:, i * LANES : (i + 1) * LANES]
            even = jnp.where(lane < SPAN, low, pltpu.roll(high, SPAN, 1)).astype(BF16)
            odd = jnp.where(lane < SPAN, pltpu.roll(low, SPAN, 1), high).astype(BF16)
            n = 4 * m + 2 * i
            scatter(n, rms(dot(even, bw[n]), gain0))
            scatter(n + 1, rms(dot(odd, bw[n + 1]), gain0))
        return carry

    lax.fori_loop(0, bands // 4, embed, 0, unroll=3)
    for n in range(bands, padded):
        scatter(n, jnp.zeros((own * frames, width), F32))

    loads[3].wait()
    loads[4].wait()
    rows = 512
    double = 2 * padded
    key = lax.broadcasted_iota(jnp.int32, (double, 2 * double), 0)
    query = lax.broadcasted_iota(jnp.int32, (double, 2 * double), 1)
    band_mask = (((key ^ query) & padded) == 0) & ((key & (padded - 1)) < bands)
    small = 8 * frames
    time_mask = (lax.broadcasted_iota(jnp.int32, (small, 2 * small), 0) & 7) == (
        lax.broadcasted_iota(jnp.int32, (small, 2 * small), 1) & 7
    )

    def out_copy(peer, b, part, slot):
        return pltpu.make_async_remote_copy(
            src_ref=sending.at[b, part, peer],
            dst_ref=out.at[slot * own + b, pl.ds(part * TIME_BANDS, TIME_BANDS)],
            send_sem=send_sem.at[b, part, peer],
            recv_sem=recv_sem.at[b, part, slot],
            device_id={"seq": peer},
            device_id_type=MESH,
        )

    def own_copy(b, part):
        return pltpu.make_async_copy(
            sending.at[b, part, me],
            out.at[me * own + b, pl.ds(part * TIME_BANDS, TIME_BANDS)],
            own_sem.at[b, part],
        )

    def one_row(b, carry):
        def band_chunk(chunk, carry):
            at = pl.multiple_of(b * frames * padded + chunk * rows, rows)
            x = jnp.concatenate(
                [x0[piece, pl.ds(at, rows), :] for piece in range(width // LANES)], axis=1
            )
            x = layer(
                x,
                (cq0[...], sq0[...], ck0[...], sk0[...]),
                gains[1:2, :],
                gains[2:3, :],
                wqkv[0],
                wout[0],
                wfi[0],
                wfo[0],
                double,
                band_mask,
                -1e30,
            )
            count = rows // padded
            x1[b, pl.ds(chunk * count, count)] = x.reshape(count, padded, width)
            return carry

        lax.fori_loop(0, frames * padded // rows, band_chunk, 0)

        def time_chunk(part, carry):
            n0 = part * TIME_BANDS
            x = jnp.concatenate(
                [
                    x1[b, :, pl.ds(pl.multiple_of(n0 + 8 * g, 8), 8), :].reshape(small, width)
                    for g in range(TIME_BANDS // 8)
                ],
                axis=0,
            )
            x = layer(
                x,
                (cq1[...], sq1[...], ck1[...], sk1[...]),
                gains[3:4, :],
                gains[4:5, :],
                wqkv[1],
                wout[1],
                wfi[1],
                wfo[1],
                small,
                time_mask,
                -1e30,
            )
            y = rms(x, gains[5:6, :])
            y = jnp.concatenate(
                [
                    y[g * small : (g + 1) * small].reshape(frames, 8, width)
                    for g in range(TIME_BANDS // 8)
                ],
                axis=1,
            )
            sending[b, part] = y.astype(BF16)

            def start(k, carry):
                peer = lax.rem(me + k, groups)
                out_copy(peer, b, part, me).start()
                return carry

            lax.fori_loop(1, groups, start, 0)
            own_copy(b, part).start()
            return carry

        lax.fori_loop(0, padded // TIME_BANDS, time_chunk, 0)
        return carry

    lax.fori_loop(0, own, one_row, 0)

    def finish_all(i, carry):
        b, part = i // 2, lax.rem(i, 2)

        def one(k, carry):
            peer = lax.rem(me + k, groups)
            copy = out_copy(peer, b, part, peer)
            copy.wait_send()
            copy.wait_recv()
            return carry

        lax.fori_loop(1, groups, one, 0)
        own_copy(b, part).wait()
        return carry

    lax.fori_loop(0, own * 2, finish_all, 0)


def batch_plan(
    spectrum,
    band_table,
    band_weight,
    qkv_weight,
    out_weight,
    ff_in_weight,
    ff_out_weight,
    norm_gains,
):
    groups = lax.axis_size("seq")
    _, batch_size, channels, bins = spectrum.shape
    bands = band_table.shape[0]
    width = band_weight.shape[3]
    hidden = ff_in_weight.shape[2]
    own = batch_size // groups
    padded = 2 * TIME_BANDS
    bins_padded = -(-bins // LANES) * LANES
    head_size = width // HEADS
    scale = math.log2(math.e) / math.sqrt(head_size)
    tables = []
    for factor in (scale, 1.0):
        for piece in rotation_tables(padded, head_size, factor):
            tables.append(np.tile(piece, (2, 1)))
    for factor in (scale, 1.0):
        for piece in rotation_tables(groups, head_size, factor):
            tables.append(np.repeat(piece, 8, axis=0))
    vmem = pl.BlockSpec(memory_space=pltpu.VMEM)
    anywhere = pl.BlockSpec(memory_space=pl.ANY)
    dma = pltpu.SemaphoreType.DMA
    out = pl.pallas_call(
        functools.partial(whole_kernel, groups, own, bands, bins),
        out_shape=jax.ShapeDtypeStruct((batch_size, padded, width), BF16),
        in_specs=[pl.BlockSpec(memory_space=pltpu.SMEM)] + [anywhere] * 6 + [vmem] * 9,
        out_specs=anywhere,
        scratch_shapes=[
            pltpu.VMEM((groups, own, channels, bins), BF16),
            pltpu.VMEM((channels * own * groups, bins_padded), F32),
            pltpu.VMEM((bands // 4, channels * own * groups, 4 * SPAN), F32),
            pltpu.VMEM((bands, channels * SPAN, width), BF16),
            pltpu.VMEM((2, width, 3 * width), BF16),
            pltpu.VMEM((2, width, width), BF16),
            pltpu.VMEM((2, width, 3 * WIDE), BF16),
            pltpu.VMEM((2, WIDE, width), BF16),
            pltpu.VMEM((2, width, hidden), BF16),
            pltpu.VMEM((2, hidden, width), BF16),
            pltpu.VMEM((width // LANES, own * groups * padded, LANES), F32),
            pltpu.VMEM((own, groups, padded, width), F32),
            pltpu.VMEM((own, 2, groups, TIME_BANDS, width), BF16),
            dma((5,)),
            dma((groups,)),
            dma((groups,)),
            dma((1,)),
            dma((own, 2, groups)),
            dma((own, 2, groups)),
            dma((own, 2)),
        ],
        compiler_params=pltpu.CompilerParams(collective_id=0, has_side_effects=True),
    )(
        band_table.T,
        spectrum.reshape(batch_size, channels, bins),
        band_weight.reshape(bands, channels * SPAN, width),
        qkv_weight,
        out_weight,
        ff_in_weight,
        ff_out_weight,
        norm_gains,
        *[jnp.asarray(t) for t in tables],
    )
    return out[None, :, :bands]


def body(
    spectrum,
    band_table,
    band_weight,
    qkv_weight,
    out_weight,
    ff_in_weight,
    ff_out_weight,
    norm_gains,
):
    frame_count, batch_size, channel_count, bin_count = spectrum.shape
    band_count = band_table.shape[0]
    if fits_batch_plan(spectrum, band_table, band_weight):
        return batch_plan(
            spectrum,
            band_table,
            band_weight,
            qkv_weight,
            out_weight,
            ff_in_weight,
            ff_out_weight,
            norm_gains,
        )
    offsets = jnp.arange(SPAN, dtype=jnp.int32)
    targets = (band_table[:, 0:1] + offsets[None, :]).reshape(-1)
    valid = (offsets[None, :] < band_table[:, 1:2]).reshape(-1)
    chosen = (
        (jnp.arange(bin_count, dtype=jnp.int32)[:, None] == targets[None, :]) & valid[None, :]
    ).astype(jnp.bfloat16)
    features = jnp.einsum(
        "fbcq,qm->fbcm", spectrum, chosen, preferred_element_type=jnp.float32
    ).astype(jnp.bfloat16)
    features = features.reshape(frame_count, batch_size, channel_count, band_count, SPAN)
    embedded = jnp.einsum(
        "fbcnj,ncjd->fbnd", features, band_weight, preferred_element_type=jnp.float32
    )
    model_width = embedded.shape[-1]
    stream = normalize(embedded, norm_gains[0]).astype(jnp.bfloat16)
    stream = stream.reshape(frame_count * batch_size, band_count, model_width)
    band_positions = jnp.arange(band_count, dtype=jnp.float32).reshape(1, band_count, 1)
    triple = project(stream, qkv_weight[0], norm_gains[1], band_positions)
    stream = finish(stream, attend_rows(triple[0], triple[1], triple[2]), out_weight[0])
    stream = feed_forward(stream, ff_in_weight[0], ff_out_weight[0], norm_gains[2])
    groups = lax.axis_size("seq")
    pair_count = batch_size * band_count
    per_group = pair_count // groups
    stream = stream.reshape(frame_count, groups, per_group, model_width)
    block = lax.all_to_all(stream, "seq", split_axis=1, concat_axis=0, tiled=True)
    flat = flatten_items(block)
    length = flat.shape[0]
    frame_positions = jnp.arange(length, dtype=jnp.float32).reshape(length, 1, 1)
    parts = project(flat, qkv_weight[1], norm_gains[3], frame_positions)
    mixed_block = finish(flat, attend_time(parts[0], parts[1], parts[2]), out_weight[1])
    result_block = feed_forward(mixed_block, ff_in_weight[1], ff_out_weight[1], norm_gains[4])
    regrouped = result_block.reshape(block.shape)
    stream = lax.all_to_all(regrouped, "seq", split_axis=0, concat_axis=1, tiled=True)
    stream = stream.reshape(frame_count, pair_count, model_width)
    result = normalize(stream.astype(jnp.float32), norm_gains[5]).astype(jnp.bfloat16)
    return result.reshape(frame_count, batch_size, band_count, model_width)


def solution(mesh):
    in_specs = (P("seq", "dp", None, None), P(), P(), P(), P(), P(), P(), P())
    out_specs = P("seq", "dp", None, None)
    return jax.shard_map(body, mesh=mesh, in_specs=in_specs, out_specs=out_specs, check_vma=False)
```

```python
import functools
import math

import jax
import jax.numpy as jnp
import numpy as np
from jax import lax
from jax.experimental import pallas as pl
from jax.experimental.pallas import tpu as pltpu
from jax.sharding import PartitionSpec as P

HEADS = 8
SPAN = 64


EPSILON = 0.05


def normalize(values, gain_row):
    return (
        values * lax.rsqrt(jnp.mean(values * values, axis=-1, keepdims=True) + EPSILON) * gain_row
    )


def rotate(tensor, positions):
    half_size = tensor.shape[-1] // 2
    frequency = 10000.0 ** (-jnp.arange(half_size, dtype=jnp.float32) / half_size)
    angles = positions[..., None] * frequency
    cosine = jnp.cos(angles)
    sine_part = jnp.sin(angles)
    first_half = tensor[..., :half_size]
    second_half = tensor[..., half_size:]
    return jnp.concatenate(
        [
            first_half * cosine - second_half * sine_part,
            second_half * cosine + first_half * sine_part,
        ],
        axis=-1,
    )


def project(stream, weights, gain_row, positions):
    normed = normalize(stream.astype(jnp.float32), gain_row).astype(jnp.bfloat16)
    mixture = jnp.dot(normed, weights, preferred_element_type=jnp.float32)
    model_width = stream.shape[-1]
    head_shape = stream.shape[:-1] + (HEADS, model_width // HEADS)
    queries = (
        rotate(mixture[..., :model_width].reshape(head_shape), positions)
        .astype(jnp.bfloat16)
        .reshape(stream.shape)
    )
    key_rows = (
        rotate(mixture[..., model_width : 2 * model_width].reshape(head_shape), positions)
        .astype(jnp.bfloat16)
        .reshape(stream.shape)
    )
    value_rows = mixture[..., 2 * model_width :].astype(jnp.bfloat16)
    return (queries, key_rows, value_rows)


def attend_rows(queries, key_rows, value_rows):
    row_count, length, model_width = queries.shape
    head_size = model_width // HEADS
    head_shape = (row_count, length, HEADS, head_size)
    scores = jnp.einsum(
        "rshd,rthd->rhst",
        queries.reshape(head_shape),
        key_rows.reshape(head_shape),
        preferred_element_type=jnp.float32,
    ) / math.sqrt(head_size)
    weights = jax.nn.softmax(scores, axis=-1).astype(jnp.bfloat16)
    context = jnp.einsum(
        "rhst,rthd->rshd",
        weights,
        value_rows.reshape(head_shape),
        preferred_element_type=jnp.float32,
    )
    return context.astype(jnp.bfloat16).reshape(row_count, length, model_width)


def attend_time(queries, key_rows, value_rows):
    context = attend_rows(
        jnp.swapaxes(queries, 0, 1), jnp.swapaxes(key_rows, 0, 1), jnp.swapaxes(value_rows, 0, 1)
    )
    return jnp.swapaxes(context, 0, 1)


def finish(stream, context, weights):
    return (
        stream.astype(jnp.float32) + jnp.dot(context, weights, preferred_element_type=jnp.float32)
    ).astype(jnp.bfloat16)


def feed_forward(stream, weight_in, weight_out, gain_row):
    normed = normalize(stream.astype(jnp.float32), gain_row).astype(jnp.bfloat16)
    active = jax.nn.gelu(
        jnp.dot(normed, weight_in, preferred_element_type=jnp.float32), approximate=True
    ).astype(jnp.bfloat16)
    return (
        stream.astype(jnp.float32) + jnp.dot(active, weight_out, preferred_element_type=jnp.float32)
    ).astype(jnp.bfloat16)


def flatten_items(block):
    return block.reshape(block.shape[0], block.shape[2], block.shape[3])


LANES = 128
PAIRS = HEADS // 2
WIDE = PAIRS * LANES
F32 = jnp.float32
BF16 = jnp.bfloat16
TIME_BANDS = 16
PADDED = 64
PARTS = PADDED // TIME_BANDS
MESH = pl.DeviceIdType.MESH


def fits_batch_plan(spectrum, band_table, band_weight):
    groups = lax.axis_size("seq")
    return (
        spectrum.shape[0] == 1
        and spectrum.shape[1] % groups == 0
        and groups % 16 == 0
        and groups <= 16
        and band_table.shape[0] <= PADDED
        and band_table.shape[0] > TIME_BANDS
        and band_table.shape[0] % 4 == 0
        and SPAN == 64
        and spectrum.shape[2] == 2
        and band_weight.shape[3] == HEADS * 48
    )


def rotation_tables(length, head_size, scale):
    half = head_size // 2
    frequency = 10000.0 ** (-np.arange(half, dtype=np.float64) / half)
    angles = np.arange(length, dtype=np.float64)[:, None] * frequency
    cosine = np.zeros((length, LANES), np.float32)
    sine = np.zeros((length, LANES), np.float32)
    for head in range(2):
        for part in range(2):
            at = part * 64 + head * 32
            cosine[:, at : at + half] = np.cos(angles) * scale
            sine[:, at : at + half] = np.sin(angles) * (scale if part else -scale)
    return cosine, sine


def dot(left, right):
    return jnp.dot(left, right, preferred_element_type=F32)


def rms(values, gain):
    mean = jnp.mean(values * values, axis=-1, keepdims=True)
    return values * lax.rsqrt(mean + EPSILON) * gain


def layer(x, tables, gain_a, gain_f, wqkv, wout, wfi, wfo, size, mask, low):
    rows = x.shape[0]
    blocks = rows // size
    cq, sq, ck, sk = tables
    lane = lax.broadcasted_iota(jnp.int32, (1, LANES), 1)
    first = ((lane & 32) == 0).astype(BF16)
    second = ((lane & 32) != 0).astype(BF16)
    normed = rms(x, gain_a).astype(BF16)
    mixture = dot(normed, wqkv)

    def turned(part, cosine, sine):
        swapped = pltpu.roll(part, 64, 1)
        part = part.reshape(blocks, size, LANES) * cosine[None]
        return (part + swapped.reshape(blocks, size, LANES) * sine[None]).astype(BF16)

    columns = []
    for pair in range(PAIRS):
        at = pair * LANES
        q = turned(mixture[:, at : at + LANES], cq, sq)
        k = turned(mixture[:, WIDE + at : WIDE + at + LANES], ck, sk)
        v = mixture[:, 2 * WIDE + at : 2 * WIDE + at + LANES].astype(BF16)
        pieces = []
        for block in range(blocks):
            qb = q[block]
            stacked = jnp.concatenate([qb * first, qb * second], axis=0)
            scores = lax.dot_general(
                k[block], stacked, (((1,), (1,)), ((), ())), preferred_element_type=F32
            )
            scores = jnp.where(mask, scores, low)
            scores = jnp.exp2(scores - jnp.max(scores, axis=0, keepdims=True))
            total = jnp.sum(scores, axis=0, keepdims=True)
            probs = (scores * (1.0 / total)).astype(BF16)
            mixed = lax.dot_general(
                probs,
                v[block * size : (block + 1) * size],
                (((0,), (0,)), ((), ())),
                preferred_element_type=F32,
            )
            pieces.append(jnp.where(lane < 64, mixed[:size], mixed[size:]))
        columns.append(jnp.concatenate(pieces, axis=0).astype(BF16))
    x = x + dot(jnp.concatenate(columns, axis=1), wout)
    normed = rms(x, gain_f).astype(BF16)
    u = dot(normed, wfi)
    c = math.sqrt(2.0 / math.pi)
    act = 0.5 * u * (1.0 + jnp.tanh(u * (c + (c * 0.044715) * (u * u))))
    return x + dot(act.astype(BF16), wfo)


def whole_kernel(
    groups,
    own,
    bands,
    bins,
    table,
    spectrum,
    band_weight,
    qkv,
    out_w,
    ff_in,
    ff_out,
    gains,
    cq0,
    sq0,
    ck0,
    sk0,
    cq1,
    sq1,
    ck1,
    sk1,
    out,
    arrived,
    spec,
    feats,
    bw,
    raw_qkv,
    raw_out,
    wqkv,
    wout,
    wfi,
    wfo,
    x0,
    x1,
    sending,
    load_sem,
    spec_send,
    spec_recv,
    spec_own,
    send_sem,
    recv_sem,
    own_sem,
):
    me = lax.axis_index("seq")
    padded = PADDED
    frames = groups
    width = gains.shape[1]
    loads = [
        pltpu.make_async_copy(qkv, raw_qkv, load_sem.at[0]),
        pltpu.make_async_copy(out_w, raw_out, load_sem.at[1]),
        pltpu.make_async_copy(band_weight, bw, load_sem.at[2]),
        pltpu.make_async_copy(ff_in, wfi, load_sem.at[3]),
        pltpu.make_async_copy(ff_out, wfo, load_sem.at[4]),
    ]
    for load in loads:
        load.start()

    barrier = pltpu.get_barrier_semaphore()

    def greet(k, carry):
        peer = lax.rem(me + k, groups)
        pl.semaphore_signal(barrier, inc=1, device_id={"seq": peer}, device_id_type=MESH)
        return carry

    lax.fori_loop(1, groups, greet, 0)
    pl.semaphore_wait(barrier, groups - 1)

    def spec_copy(peer, slot, sem_slot):
        return pltpu.make_async_remote_copy(
            src_ref=spectrum.at[pl.ds(peer * own, own)],
            dst_ref=arrived.at[slot],
            send_sem=spec_send.at[peer],
            recv_sem=spec_recv.at[sem_slot],
            device_id={"seq": peer},
            device_id_type=MESH,
        )

    def spec_start(k, carry):
        peer = lax.rem(me + k, groups)
        spec_copy(peer, me, me).start()
        return carry

    lax.fori_loop(1, groups, spec_start, 0)
    tail = bins // LANES * LANES
    spec[:, tail:] = jnp.zeros((spec.shape[0], spec.shape[1] - tail), F32)
    mine = pltpu.make_async_copy(
        spectrum.at[pl.ds(me * own, own)], arrived.at[me], spec_own.at[0]
    )
    mine.start()

    col = lax.broadcasted_iota(jnp.int32, (1, WIDE), 1)
    pair, rest = col >> 7, col & 127
    part, head, at = rest >> 6, (rest >> 5) & 1, rest & 31
    source = jnp.where(at < 24, pair * 96 + head * 48 + part * 24 + at, -1)
    row = lax.broadcasted_iota(jnp.int32, (width, WIDE), 0)
    spread_qk = (row == source).astype(F32).astype(BF16)
    source = jnp.where((col & 63) < 48, (col >> 6) * 48 + (col & 63), -1)
    spread_v = (row == source).astype(F32).astype(BF16)
    col = lax.broadcasted_iota(jnp.int32, (WIDE, 1), 0)
    source = jnp.where((col & 63) < 48, (col >> 6) * 48 + (col & 63), -1)
    row = lax.broadcasted_iota(jnp.int32, (WIDE, width), 1)
    spread_o = (row == source).astype(F32).astype(BF16)
    loads[0].wait()
    loads[1].wait()
    for sub in range(2):
        for block in range(3):
            spread = spread_v if block == 2 else spread_qk
            wqkv[sub, :, block * WIDE : (block + 1) * WIDE] = dot(
                raw_qkv[sub, :, block * width : (block + 1) * width], spread
            ).astype(BF16)
        wout[sub] = dot(spread_o, raw_out[sub]).astype(BF16)

    mine.wait()

    def spec_wait(k, carry):
        peer = lax.rem(me + k, groups)
        copy = spec_copy(peer, peer, peer)
        copy.wait_send()
        copy.wait_recv()
        return carry

    lax.fori_loop(1, groups, spec_wait, 0)
    for f in range(frames):
        for b in range(own):
            both = arrived[f, b].astype(F32)
            at = b * frames + f
            spec[at : at + 1, 0:bins] = both[0:1]
            at = (own + b) * frames + f
            spec[at : at + 1, 0:bins] = both[1:2]

    loads[2].wait()
    lane = lax.broadcasted_iota(jnp.int32, (1, LANES), 1)
    gain0 = gains[0:1, :]

    def scatter(n, values):
        for b in range(own):
            for piece in range(width // LANES):
                x0[piece, pl.ds(b * frames * padded + n, frames, stride=padded), :] = values[
                    b * frames : (b + 1) * frames, piece * LANES : (piece + 1) * LANES
                ]

    quad = 4 * SPAN
    offset = lax.broadcasted_iota(jnp.int32, (1, quad), 1) & (SPAN - 1)
    owner = lax.broadcasted_iota(jnp.int32, (1, quad), 1) // SPAN
    lines = spec[...].astype(BF16)
    bin_row = lax.broadcasted_iota(jnp.int32, (spec.shape[1], quad), 0)

    def pick(m, carry):
        target = jnp.full((1, quad), -1, jnp.int32)
        for i in range(4):
            start = jnp.full((1, quad), table[0, 4 * m + i], jnp.int32)
            count = jnp.full((1, quad), table[1, 4 * m + i], jnp.int32)
            inside = (owner == i) & (offset < count)
            target = jnp.where(inside, start + offset, target)
        chosen = (bin_row == target).astype(F32).astype(BF16)
        feats[m] = dot(lines, chosen)
        return carry

    lax.fori_loop(0, bands // 4, pick, 0, unroll=3)
    half = own * frames

    def embed(m, carry):
        for i in range(2):
            low = feats[m, :half, i * LANES : (i + 1) * LANES]
            high = feats[m, half:, i * LANES : (i + 1) * LANES]
            even = jnp.where(lane < SPAN, low, pltpu.roll(high, SPAN, 1)).astype(BF16)
            odd = jnp.where(lane < SPAN, pltpu.roll(low, SPAN, 1), high).astype(BF16)
            n = 4 * m + 2 * i
            scatter(n, rms(dot(even, bw[n]), gain0))
            scatter(n + 1, rms(dot(odd, bw[n + 1]), gain0))
        return carry

    lax.fori_loop(0, bands // 4, embed, 0, unroll=3)
    for n in range(bands, padded):
        scatter(n, jnp.zeros((own * frames, width), F32))

    loads[3].wait()
    loads[4].wait()
    rows = 512
    double = 2 * padded
    key = lax.broadcasted_iota(jnp.int32, (double, 2 * double), 0)
    query = lax.broadcasted_iota(jnp.int32, (double, 2 * double), 1)
    band_mask = (((key ^ query) & padded) == 0) & ((key & (padded - 1)) < bands)
    small = 8 * frames
    time_mask = (lax.broadcasted_iota(jnp.int32, (small, 2 * small), 0) & 7) == (
        lax.broadcasted_iota(jnp.int32, (small, 2 * small), 1) & 7
    )

    def out_copy(peer, b, part, slot):
        return pltpu.make_async_remote_copy(
            src_ref=sending.at[b, part, peer],
            dst_ref=out.at[slot * own + b, pl.ds(part * TIME_BANDS, TIME_BANDS)],
            send_sem=send_sem.at[b, part, peer],
            recv_sem=recv_sem.at[b, part, slot],
            device_id={"seq": peer},
            device_id_type=MESH,
        )

    def own_copy(b, part):
        return pltpu.make_async_copy(
            sending.at[b, part, me],
            out.at[me * own + b, pl.ds(part * TIME_BANDS, TIME_BANDS)],
            own_sem.at[b, part],
        )

    def one_row(b, carry):
        def band_chunk(chunk, carry):
            at = pl.multiple_of(b * frames * padded + chunk * rows, rows)
            x = jnp.concatenate(
                [x0[piece, pl.ds(at, rows), :] for piece in range(width // LANES)], axis=1
            )
            x = layer(
                x,
                (cq0[...], sq0[...], ck0[...], sk0[...]),
                gains[1:2, :],
                gains[2:3, :],
                wqkv[0],
                wout[0],
                wfi[0],
                wfo[0],
                double,
                band_mask,
                -1e30,
            )
            count = rows // padded
            x1[b, pl.ds(chunk * count, count)] = x.reshape(count, padded, width)
            return carry

        lax.fori_loop(0, frames * padded // rows, band_chunk, 0)

        def time_chunk(part, carry):
            n0 = part * TIME_BANDS
            x = jnp.concatenate(
                [
                    x1[b, :, pl.ds(pl.multiple_of(n0 + 8 * g, 8), 8), :].reshape(small, width)
                    for g in range(TIME_BANDS // 8)
                ],
                axis=0,
            )
            x = layer(
                x,
                (cq1[...], sq1[...], ck1[...], sk1[...]),
                gains[3:4, :],
                gains[4:5, :],
                wqkv[1],
                wout[1],
                wfi[1],
                wfo[1],
                small,
                time_mask,
                -1e30,
            )
            y = rms(x, gains[5:6, :])
            y = jnp.concatenate(
                [
                    y[g * small : (g + 1) * small].reshape(frames, 8, width)
                    for g in range(TIME_BANDS // 8)
                ],
                axis=1,
            )
            sending[b, part] = y.astype(BF16)

            def start(k, carry):
                peer = lax.rem(me + k, groups)
                out_copy(peer, b, part, me).start()
                return carry

            lax.fori_loop(1, groups, start, 0)
            own_copy(b, part).start()
            return carry

        lax.fori_loop(0, padded // TIME_BANDS, time_chunk, 0)
        return carry

    lax.fori_loop(0, own, one_row, 0)

    def finish_all(i, carry):
        b, part = i // PARTS, lax.rem(i, PARTS)

        def one(k, carry):
            peer = lax.rem(me + k, groups)
            copy = out_copy(peer, b, part, peer)
            copy.wait_send()
            copy.wait_recv()
            return carry

        lax.fori_loop(1, groups, one, 0)
        own_copy(b, part).wait()
        return carry

    lax.fori_loop(0, own * PARTS, finish_all, 0)


def batch_plan(
    spectrum,
    band_table,
    band_weight,
    qkv_weight,
    out_weight,
    ff_in_weight,
    ff_out_weight,
    norm_gains,
):
    groups = lax.axis_size("seq")
    _, batch_size, channels, bins = spectrum.shape
    bands = band_table.shape[0]
    width = band_weight.shape[3]
    hidden = ff_in_weight.shape[2]
    own = batch_size // groups
    padded = PADDED
    bins_padded = -(-bins // LANES) * LANES
    head_size = width // HEADS
    scale = math.log2(math.e) / math.sqrt(head_size)
    tables = []
    for factor in (scale, 1.0):
        for piece in rotation_tables(padded, head_size, factor):
            tables.append(np.tile(piece, (2, 1)))
    for factor in (scale, 1.0):
        for piece in rotation_tables(groups, head_size, factor):
            tables.append(np.repeat(piece, 8, axis=0))
    vmem = pl.BlockSpec(memory_space=pltpu.VMEM)
    anywhere = pl.BlockSpec(memory_space=pl.ANY)
    dma = pltpu.SemaphoreType.DMA
    out = pl.pallas_call(
        functools.partial(whole_kernel, groups, own, bands, bins),
        out_shape=jax.ShapeDtypeStruct((batch_size, padded, width), BF16),
        in_specs=[pl.BlockSpec(memory_space=pltpu.SMEM)] + [anywhere] * 6 + [vmem] * 9,
        out_specs=anywhere,
        scratch_shapes=[
            pltpu.VMEM((groups, own, channels, bins), BF16),
            pltpu.VMEM((channels * own * groups, bins_padded), F32),
            pltpu.VMEM((bands // 4, channels * own * groups, 4 * SPAN), F32),
            pltpu.VMEM((bands, channels * SPAN, width), BF16),
            pltpu.VMEM((2, width, 3 * width), BF16),
            pltpu.VMEM((2, width, width), BF16),
            pltpu.VMEM((2, width, 3 * WIDE), BF16),
            pltpu.VMEM((2, WIDE, width), BF16),
            pltpu.VMEM((2, width, hidden), BF16),
            pltpu.VMEM((2, hidden, width), BF16),
            pltpu.VMEM((width // LANES, own * groups * padded, LANES), F32),
            pltpu.VMEM((own, groups, padded, width), F32),
            pltpu.VMEM((own, PARTS, groups, TIME_BANDS, width), BF16),
            dma((5,)),
            dma((groups,)),
            dma((groups,)),
            dma((1,)),
            dma((own, PARTS, groups)),
            dma((own, PARTS, groups)),
            dma((own, PARTS)),
        ],
        compiler_params=pltpu.CompilerParams(collective_id=0, has_side_effects=True),
    )(
        band_table.T,
        spectrum.reshape(batch_size, channels, bins),
        band_weight.reshape(bands, channels * SPAN, width),
        qkv_weight,
        out_weight,
        ff_in_weight,
        ff_out_weight,
        norm_gains,
        *[jnp.asarray(t) for t in tables],
    )
    return out[None, :, :bands]


def body(
    spectrum,
    band_table,
    band_weight,
    qkv_weight,
    out_weight,
    ff_in_weight,
    ff_out_weight,
    norm_gains,
):
    frame_count, batch_size, channel_count, bin_count = spectrum.shape
    band_count = band_table.shape[0]
    if fits_batch_plan(spectrum, band_table, band_weight):
        return batch_plan(
            spectrum,
            band_table,
            band_weight,
            qkv_weight,
            out_weight,
            ff_in_weight,
            ff_out_weight,
            norm_gains,
        )
    offsets = jnp.arange(SPAN, dtype=jnp.int32)
    targets = (band_table[:, 0:1] + offsets[None, :]).reshape(-1)
    valid = (offsets[None, :] < band_table[:, 1:2]).reshape(-1)
    chosen = (
        (jnp.arange(bin_count, dtype=jnp.int32)[:, None] == targets[None, :]) & valid[None, :]
    ).astype(jnp.bfloat16)
    features = jnp.einsum(
        "fbcq,qm->fbcm", spectrum, chosen, preferred_element_type=jnp.float32
    ).astype(jnp.bfloat16)
    features = features.reshape(frame_count, batch_size, channel_count, band_count, SPAN)
    embedded = jnp.einsum(
        "fbcnj,ncjd->fbnd", features, band_weight, preferred_element_type=jnp.float32
    )
    model_width = embedded.shape[-1]
    stream = normalize(embedded, norm_gains[0]).astype(jnp.bfloat16)
    stream = stream.reshape(frame_count * batch_size, band_count, model_width)
    band_positions = jnp.arange(band_count, dtype=jnp.float32).reshape(1, band_count, 1)
    triple = project(stream, qkv_weight[0], norm_gains[1], band_positions)
    stream = finish(stream, attend_rows(triple[0], triple[1], triple[2]), out_weight[0])
    stream = feed_forward(stream, ff_in_weight[0], ff_out_weight[0], norm_gains[2])
    groups = lax.axis_size("seq")
    pair_count = batch_size * band_count
    per_group = pair_count // groups
    stream = stream.reshape(frame_count, groups, per_group, model_width)
    block = lax.all_to_all(stream, "seq", split_axis=1, concat_axis=0, tiled=True)
    flat = flatten_items(block)
    length = flat.shape[0]
    frame_positions = jnp.arange(length, dtype=jnp.float32).reshape(length, 1, 1)
    parts = project(flat, qkv_weight[1], norm_gains[3], frame_positions)
    mixed_block = finish(flat, attend_time(parts[0], parts[1], parts[2]), out_weight[1])
    result_block = feed_forward(mixed_block, ff_in_weight[1], ff_out_weight[1], norm_gains[4])
    regrouped = result_block.reshape(block.shape)
    stream = lax.all_to_all(regrouped, "seq", split_axis=0, concat_axis=1, tiled=True)
    stream = stream.reshape(frame_count, pair_count, model_width)
    result = normalize(stream.astype(jnp.float32), norm_gains[5]).astype(jnp.bfloat16)
    return result.reshape(frame_count, batch_size, band_count, model_width)


def solution(mesh):
    in_specs = (P("seq", "dp", None, None), P(), P(), P(), P(), P(), P(), P())
    out_specs = P("seq", "dp", None, None)
    return jax.shard_map(body, mesh=mesh, in_specs=in_specs, out_specs=out_specs, check_vma=False)
```
